8 devices in a mesh: by: 4 (over z, y, x), bx: 2 (over core).
Axes of the slice: x: 2, y: 2, z: 1, core: 2. Of those that a mesh axis runs over, the one named last changes fastest.
Arguments:
- wave_fn: float32 [3072, 2, 2, 3072], P('bx', None, None, 'by')
- left_env: float32 [3072, 3, 3072], P('bx')
- mpo_ten: float32 [3, 2, 2, 3], replicated
- right_env: float32 [3072, 3, 3072], P('by')
Outputs:
- output: float32 [3072, 2, 2, 3072], P('bx', None, None, 'by')
All inputs are finite; a program needn't handle non-finite values.
Results may differ from the reference program's by a relative error of at most 0.001.
Values sent between devices are 32-bit elements.
A program may use at most 1 GiB of HBM per device.

```python
import jax
import jax.numpy as jnp
from jax import lax

BOND_DIM = 3072
PHYS_DIM = 2
MPO_DIM = 3


def setup_inputs(seed: int = 0) -> dict:
    key = jax.random.key(seed)
    k_wave, k_left, k_mpo, k_right = jax.random.split(key, 4)
    wave_fn = jax.random.normal(k_wave, (BOND_DIM, PHYS_DIM, PHYS_DIM, BOND_DIM), jnp.float32)
    left_env = jax.random.normal(k_left, (BOND_DIM, MPO_DIM, BOND_DIM), jnp.float32) * (BOND_DIM ** -0.5)
    mpo_ten = jax.random.normal(k_mpo, (MPO_DIM, PHYS_DIM, PHYS_DIM, MPO_DIM), jnp.float32) * ((MPO_DIM * PHYS_DIM) ** -0.5)
    right_env = jax.random.normal(k_right, (BOND_DIM, MPO_DIM, BOND_DIM), jnp.float32) * ((MPO_DIM * BOND_DIM) ** -0.5)
    return {'wave_fn': wave_fn, 'left_env': left_env, 'mpo_ten': mpo_ten, 'right_env': right_env}


def reference(wave_fn, left_env, mpo_ten, right_env):
    row_block = min(BOND_DIM, 128)
    block_count = BOND_DIM // row_block
    left_blocks = left_env.reshape(block_count, row_block, MPO_DIM, BOND_DIM)

    def one_block(left_rows):
        stage_one = jnp.einsum('auc,cpqf->aupqf', left_rows.astype(jnp.float32), wave_fn.astype(jnp.float32))
        stage_two = jnp.einsum('aupqf,uspv->asvqf', stage_one, mpo_ten.astype(jnp.float32))
        stage_three = jnp.einsum('asvqf,vtqr->astrf', stage_two, mpo_ten.astype(jnp.float32))
        return jnp.einsum('astrf,brf->astb', stage_three, right_env.astype(jnp.float32))

    out_blocks = lax.map(one_block, left_blocks)
    return out_blocks.reshape(BOND_DIM, PHYS_DIM, PHYS_DIM, BOND_DIM)
```

```python
import jax
import jax.numpy as jnp
from jax import lax
from jax.experimental import pallas as pl
from jax.experimental.pallas import tpu as pltpu
from jax.sharding import PartitionSpec as P

F32 = jnp.float32
BF16 = jnp.bfloat16
LANES = 128
BLK = 256
VMEM_LIMIT = 62 * 2**20


def limbs(val):
    hi = val.astype(BF16)
    rest = val - hi.astype(F32)
    mid = rest.astype(BF16)
    return hi, mid, (rest - mid.astype(F32)).astype(BF16)


def full_product(acc, unit, lhs_limbs, rhs_limbs, transpose, reg):
    for depth, rhs in enumerate(rhs_limbs):
        pltpu.matmul_push_rhs(rhs, staging_register=reg, mxu_index=unit, transpose=transpose)
        for i in range(3 - depth):
            pltpu.matmul_acc_lhs(acc, lhs_limbs[i], load_staged_rhs=reg if i == 0 else None)
        reg = 1 - reg
    return reg


def wave_limbs(lines, k, buf, rows):
    for p in range(2):
        for q in range(2):
            for half in range(2):
                part = lines[2 * k + half, pl.ds(2 * p + q, rows, stride=4), :]
                for i, limb in enumerate(limbs(part)):
                    buf[i, p, q * rows:(q + 1) * rows, half * LANES:(half + 1) * LANES] = limb


def first_products(env_of, buf, accs, reg):
    for r in range(3):
        env = limbs(env_of(r))
        start = reg
        for p in range(2):
            reg = full_product(accs[p][r], p, [buf[i, p] for i in range(3)], env, True, start)
    return reg


def acc_refs(rows, count):
    return tuple(pltpu.ACC(unit)((rows, BLK), F32) for unit in range(2) for _ in range(count))


CT = 128
LINE_CT = 64


def to_lines_kernel(bounds, wave, *outs):
    step = pl.program_id(0)
    for out, (lo, hi) in zip(outs, bounds):
        @pl.when((step >= lo) & (step < hi))
        def _():
            for f in range(6):
                out[f] = wave[:, :, :, f * LANES:(f + 1) * LANES].reshape(LINE_CT * 4, LANES)


def from_lines_kernel(lines, out):
    for f in range(6):
        out[:, :, :, f * LANES:(f + 1) * LANES] = lines[f].reshape(LINE_CT, 2, 2, LANES)


def local_kernel(wave, right, part, lines, buf_a, buf_b, buf_c):
    bufs = (buf_a, buf_b, buf_c)

    def prepare(k):
        for f in (2 * k, 2 * k + 1):
            lines[f] = wave[:, :, :, f * LANES:(f + 1) * LANES].reshape(CT * 4, LANES)
        wave_limbs(lines, k, bufs[k], CT)

    def run(*refs):
        accs = (refs[:3], refs[3:])
        reg = 0
        prepare(0)
        for b in range(3):
            for k in range(3):
                if b == 0 and k < 2:
                    prepare(k + 1)
                reg = first_products(lambda r: right[r, b * BLK:(b + 1) * BLK, k * BLK:(k + 1) * BLK], bufs[k], accs, reg)
            for r in range(3):
                for p in range(2):
                    got = pltpu.matmul_pop(accs[p][r])
                    for q in range(2):
                        part[(p * 2 + q) * 3 + r, :, b * BLK:(b + 1) * BLK] = got[q * CT:(q + 1) * CT]

    pl.run_scoped(run, *acc_refs(2 * CT, 3))


def mix_rows(w, mid, out, row):
    rows = pl.ds(row, 8)
    for h in range(2):
        cols = slice(h * LANES, (h + 1) * LANES)
        halves = {}
        for p in range(2):
            x2 = [mid[p * 6 + i, rows, cols] for i in range(6)]
            for v in range(3):
                for t in range(2):
                    halves[v, t, p] = sum(w[v, t, q, r] * x2[q * 3 + r] for q in range(2) for r in range(3))
        for t in range(2):
            for u in range(3):
                for s in range(2):
                    out[u, s * 2 + t, rows, cols] = sum(w[u, s, p, v] * halves[v, t, p] for p in range(2) for v in range(3))


def site_tensor(w_ref):
    return {(u, s, p, v): w_ref[((u * 2 + s) * 2 + p) * 3 + v]
            for u in range(3) for s in range(2) for p in range(2) for v in range(3)}


def remote_kernel(n_tiles, own_ref, w_ref, wave, right, part, out, buf_a, buf_b, buf_c, mid):
    bufs = (buf_a, buf_b, buf_c)
    step = pl.program_id(0)
    own = own_ref[0]
    w = site_tensor(w_ref)
    groups = CT // 8

    def run(*refs):
        accs = (refs[:3], refs[3:])

        @pl.when(step < n_tiles)
        def _():
            wave_limbs(wave.at[lax.rem(own + 1, 4)], 0, bufs[0], CT)

            def shard_step(m, carry):
                shard = lax.rem(own + 1 + m, 4)
                later = lax.rem(own + 1 + jnp.minimum(m + 1, 2), 4)
                reg = 0
                for k in range(3):
                    if k < 2:
                        wave_limbs(wave.at[shard], k + 1, bufs[k + 1], CT)
                    else:
                        wave_limbs(wave.at[later], 0, bufs[0], CT)
                    for g in range(2):
                        row = jnp.minimum(m * 6 + k * 2 + g, groups - 1) * 8
                        mix_rows(w, mid, out, pl.multiple_of(row, 8))
                    first = pl.multiple_of(shard * 768 + k * BLK, BLK)
                    reg = first_products(lambda r: right[r, :, pl.ds(first, BLK)], bufs[k], accs, reg)
                return carry

            lax.fori_loop(0, 3, shard_step, 0)
            for r in range(3):
                for p in range(2):
                    got = pltpu.matmul_pop(accs[p][r])
                    for q in range(2):
                        i = (p * 2 + q) * 3 + r
                        mid[i] = got[q * CT:(q + 1) * CT] + part[i]

        @pl.when(step == n_tiles)
        def _():
            def group(g, carry):
                mix_rows(w, mid, out, pl.multiple_of(g * 8, 8))
                return carry

            lax.fori_loop(0, groups, group, 0)

    pl.run_scoped(run, *acc_refs(2 * CT, 3))


AT = 768


def second_kernel(n_src, has_prev, final, *refs):
    lefts, zs, refs = refs[:n_src], refs[n_src:2 * n_src], refs[2 * n_src:]
    prev, refs = (refs[0], refs[1:]) if has_prev else (None, refs)
    out, buf_a, buf_b = refs
    bufs = (buf_a, buf_b)
    col = pl.program_id(1)

    def run(acc0, acc1):
        steps = [(m, u) for m in range(n_src) for u in range(3)]

        def left_limbs(n):
            m, u = steps[n]
            for i, limb in enumerate(limbs(lefts[m][u])):
                bufs[n % 2][i] = limb

        left_limbs(0)
        reg = 0
        for n, (m, u) in enumerate(steps):
            if n + 1 < len(steps):
                left_limbs(n + 1)
            start = reg
            for t, acc in enumerate((acc0, acc1)):
                reg = full_product(acc, t, [bufs[n % 2][i] for i in range(3)], limbs(zs[m][u, t]), False, start)
        for t, acc in enumerate((acc0, acc1)):
            got = pltpu.matmul_pop(acc)
            if has_prev:
                got = got + prev[:, t * BLK:(t + 1) * BLK]
            if final:
                for half in range(2):
                    out[half, pl.ds(2 * (col % 2) + t, AT, stride=4), :] = got[:, half * LANES:(half + 1) * LANES]
            else:
                out[:, t * BLK:(t + 1) * BLK] = got

    pl.run_scoped(run, pltpu.ACC(0)((AT, BLK), F32), pltpu.ACC(1)((AT, BLK), F32))


def params():
    return pltpu.CompilerParams(vmem_limit_bytes=VMEM_LIMIT)


def cost(flops, nbytes):
    return pl.CostEstimate(flops=flops, bytes_accessed=nbytes, transcendentals=0)


def solution(mesh):
    def local_apply(wave_blk, left_rows, mpo_ten, right_rows):
        rows_c, cols_f = wave_blk.shape[0], wave_blk.shape[3]
        n_by = 4
        chunk = 256
        n_chunk = rows_c // chunk
        tiles = chunk // CT
        by, bx = lax.axis_index('by'), lax.axis_index('bx')
        left = left_rows.transpose(1, 0, 2)
        right = right_rows.transpose(1, 0, 2)
        mpo_flat = mpo_ten.reshape(-1)
        own = by.astype(jnp.int32)[None]
        line_steps = chunk // LINE_CT

        def to_lines(lo, hi):
            n = hi - lo
            bounds = [(j * line_steps, (j + 1) * line_steps) for j in range(n)]
            return pl.pallas_call(
                lambda *refs: to_lines_kernel(bounds, *refs),
                grid=(n * line_steps,),
                in_specs=[pl.BlockSpec((LINE_CT, 2, 2, cols_f), lambda i: (lo * line_steps + i, 0, 0, 0))],
                out_specs=[pl.BlockSpec((6, LINE_CT * 4, LANES), lambda i, j=j: (0, jnp.clip(i - j * line_steps, 0, line_steps - 1), 0)) for j in range(n)],
                out_shape=[jax.ShapeDtypeStruct((6, chunk * 4, LANES), F32)] * n,
                compiler_params=params(),
                cost_estimate=cost(10**9 * n, 8 * n * 2**20),
                name='to_lines',
            )(wave_blk)

        lines = to_lines(0, 1) + to_lines(1, n_chunk)
        gathered = [lax.all_gather(line, 'by', axis=0, tiled=False) for line in lines]

        part = pl.pallas_call(
            lambda idx, *refs: local_kernel(*refs),
            grid_spec=pltpu.PrefetchScalarGridSpec(
                num_scalar_prefetch=1,
                grid=(rows_c // CT,),
                in_specs=[
                    pl.BlockSpec((CT, 2, 2, cols_f), lambda i, idx: (i, 0, 0, 0)),
                    pl.BlockSpec((3, 768, 768), lambda i, idx: (0, 0, idx[0]), pipeline_mode=pl.Buffered(1)),
                ],
                out_specs=pl.BlockSpec((12, CT, 768), lambda i, idx: (0, i, 0)),
                scratch_shapes=[pltpu.VMEM((6, CT * 4, LANES), F32)] + [pltpu.VMEM((3, 2, 2 * CT, BLK), BF16)] * 3,
            ),
            out_shape=jax.ShapeDtypeStruct((12, rows_c, 768), F32),
            compiler_params=params(),
            cost_estimate=cost(2 * rows_c * 4 * 768 * 2304 * 6, 120 * 2**20),
            name='local_part',
        )(own, wave_blk, right)

        def first(k, got):
            n_tiles = tiles * 3

            def tile(i):
                return jnp.minimum(i, n_tiles - 1)

            def done(i):
                return jnp.maximum(i - 1, 0)

            return pl.pallas_call(
                lambda *refs: remote_kernel(n_tiles, *refs),
                grid_spec=pltpu.PrefetchScalarGridSpec(
                    num_scalar_prefetch=1,
                    grid=(n_tiles + 1,),
                    in_specs=[
                        pl.BlockSpec(memory_space=pltpu.SMEM),
                        pl.BlockSpec((4, 6, CT * 4, LANES), lambda i, idx: (0, 0, tile(i) % tiles, 0)),
                        pl.BlockSpec((3, BLK, 3072), lambda i, idx: (0, tile(i) // tiles, 0)),
                        pl.BlockSpec((12, CT, BLK), lambda i, idx: (0, k * tiles + tile(i) % tiles, tile(i) // tiles)),
                    ],
                    out_specs=pl.BlockSpec((3, 4, CT, BLK), lambda i, idx: (0, 0, done(i) % tiles, done(i) // tiles)),
                    scratch_shapes=[pltpu.VMEM((3, 2, 2 * CT, BLK), BF16)] * 3 + [pltpu.VMEM((12, CT, BLK), F32)],
                ),
                out_shape=jax.ShapeDtypeStruct((3, 4, chunk, 768), F32),
                compiler_params=params(),
                cost_estimate=cost(2 * chunk * 4 * 2304 * 2304 * 6, 60 * 2**20),
                name='remote_part',
            )(own, mpo_flat, got, right, part)

        def second(group, mine, theirs, prev, final):
            srcs = [(bx, k) for k in group] + [(1 - bx, k) for k in group]
            where = jnp.stack([b * n_chunk + k for b, k in srcs]).astype(jnp.int32)
            n_src = len(srcs)
            in_specs = [pl.BlockSpec((3, AT, chunk), lambda a, n, idx, m=m: (0, a, idx[m])) for m in range(n_src)]
            in_specs += [pl.BlockSpec((3, 2, chunk, BLK), lambda a, n, idx: (0, n % 2, 0, n // 2))] * n_src
            operands = [left] * n_src + mine + theirs
            if prev is not None:
                in_specs.append(pl.BlockSpec((AT, 2 * BLK), lambda a, n, idx: (a, n)))
                operands.append(prev)
            if final:
                out_spec = pl.BlockSpec((2, AT * 4, LANES), lambda a, n, idx: (n // 2, a, 0))
                out_shape = jax.ShapeDtypeStruct((6, rows_c * 4, LANES), F32)
            else:
                out_spec = pl.BlockSpec((AT, 2 * BLK), lambda a, n, idx: (a, n))
                out_shape = jax.ShapeDtypeStruct((rows_c, 3072), F32)
            return pl.pallas_call(
                lambda idx, *refs: second_kernel(n_src, prev is not None, final, *refs),
                grid_spec=pltpu.PrefetchScalarGridSpec(
                    num_scalar_prefetch=1,
                    grid=(rows_c // AT, 6),
                    in_specs=in_specs,
                    out_specs=out_spec,
                    scratch_shapes=[pltpu.VMEM((3, AT, BLK), BF16)] * 2,
                ),
                out_shape=out_shape,
                compiler_params=params(),
                cost_estimate=cost(2 * rows_c * 3072 * 3 * chunk * n_src * 6, 100 * 2**20),
                name='second_part',
            )(where, *operands)

        mine, theirs = [], []

        def stage(k):
            z = first(k, gathered[k])
            mine.append(z)
            theirs.append(lax.ppermute(z, 'bx', [(0, 1), (1, 0)]))

        def apply(group, prev, final):
            return second(group, [mine[k] for k in group], [theirs[k] for k in group], prev, final)

        def after(k, val):
            gathered[k], val = lax.optimization_barrier((gathered[k], val))
            return val

        stage(0)
        stage(1)
        acc = apply([0], None, False)
        acc = after(2, acc)
        stage(2)
        stage(3)
        acc = apply([1, 2], acc, False)
        acc = after(4, acc)
        stage(4)
        stage(5)
        acc = apply([3, 4], acc, False)
        acc = apply([5], acc, True)
        return pl.pallas_call(
            from_lines_kernel,
            grid=(rows_c // LINE_CT,),
            in_specs=[pl.BlockSpec((6, LINE_CT * 4, LANES), lambda i: (0, i, 0))],
            out_specs=pl.BlockSpec((LINE_CT, 2, 2, cols_f), lambda i: (i, 0, 0, 0)),
            out_shape=jax.ShapeDtypeStruct((rows_c, 2, 2, cols_f), F32),
            compiler_params=params(),
            name='from_lines',
        )(acc)

    return jax.shard_map(local_apply, mesh=mesh, in_specs=(P('bx', None, None, 'by'), P('bx', None, None), P(), P('by', None, None)), out_specs=P('bx', None, None, 'by'), check_vma=False)
```

```python
import jax
import jax.numpy as jnp
from jax import lax
from jax.experimental import pallas as pl
from jax.experimental.pallas import tpu as pltpu
from jax.sharding import PartitionSpec as P

F32 = jnp.float32
BF16 = jnp.bfloat16
LANES = 128
BLK = 256
VMEM_LIMIT = 62 * 2**20


def limbs(val):
    hi = val.astype(BF16)
    rest = val - hi.astype(F32)
    mid = rest.astype(BF16)
    return hi, mid, (rest - mid.astype(F32)).astype(BF16)


def full_product(acc, unit, lhs_limbs, rhs_limbs, transpose, reg):
    for depth, rhs in enumerate(rhs_limbs):
        pltpu.matmul_push_rhs(rhs, staging_register=reg, mxu_index=unit, transpose=transpose)
        for i in range(3 - depth):
            pltpu.matmul_acc_lhs(acc, lhs_limbs[i], load_staged_rhs=reg if i == 0 else None)
        reg = 1 - reg
    return reg


PIECE = 64


def wave_limbs(lines, k, buf, rows):
    for p in range(2):
        for q in range(2):
            for top in range(0, rows, PIECE):
                for half in range(2):
                    part = lines[2 * k + half, pl.ds(4 * top + 2 * p + q, PIECE, stride=4), :]
                    for i, limb in enumerate(limbs(part)):
                        buf[i, p, q * rows + top:q * rows + top + PIECE, half * LANES:(half + 1) * LANES] = limb


def first_products(env_of, buf, accs, reg):
    for r in range(3):
        env = limbs(env_of(r))
        start = reg
        for p in range(2):
            reg = full_product(accs[p][r], p, [buf[i, p] for i in range(3)], env, True, start)
    return reg


def acc_refs(rows, count):
    return tuple(pltpu.ACC(unit)((rows, BLK), F32) for unit in range(2) for _ in range(count))


CT = 128
LINE_CT = 128


def line_copies(wave, first, rows, lines, sems):
    return [
        pltpu.make_async_copy(
            wave.at[pl.ds(first, rows), :, :, pl.ds(f * LANES, LANES)], lines.at[f].reshape(rows, 2, 2, LANES), sems.at[f])
        for f in range(6)
    ]


def to_lines_kernel(base, bounds, wave, *refs):
    outs, sems = refs[:-1], refs[-1]
    step = pl.program_id(0)
    for out, (lo, hi) in zip(outs, bounds):
        @pl.when((step >= lo) & (step < hi))
        def _():
            copies = line_copies(wave, base + step * LINE_CT, LINE_CT, out, sems)
            for copy in copies:
                copy.start()
            for copy in copies:
                copy.wait()


def local_kernel(n_tiles, wave, right, part, lines, sems, buf_a, buf_b, buf_c):
    bufs = (buf_a, buf_b, buf_c)
    step = pl.program_id(0)
    slot = lax.rem(step, 2)

    def copies(tile, at):
        return line_copies(wave, tile * CT, CT, lines.at[at], sems.at[at])

    @pl.when(step == 0)
    def _():
        for copy in copies(0, 0):
            copy.start()

    @pl.when(step + 1 < n_tiles)
    def _():
        for copy in copies(step + 1, 1 - slot):
            copy.start()

    for copy in copies(step, slot):
        copy.wait()
    here = lines.at[slot]

    def run(*refs):
        accs = (refs[:3], refs[3:])
        reg = 0
        wave_limbs(here, 0, bufs[0], CT)
        for b in range(3):
            for k in range(3):
                if b == 0 and k < 2:
                    wave_limbs(here, k + 1, bufs[k + 1], CT)
                reg = first_products(lambda r: right[r, b * BLK:(b + 1) * BLK, k * BLK:(k + 1) * BLK], bufs[k], accs, reg)
            for r in range(3):
                for p in range(2):
                    got = pltpu.matmul_pop(accs[p][r])
                    for q in range(2):
                        part[(p * 2 + q) * 3 + r, :, b * BLK:(b + 1) * BLK] = got[q * CT:(q + 1) * CT]

    pl.run_scoped(run, *acc_refs(2 * CT, 3))


def mix_rows(w, mid, out, row):
    rows = pl.ds(row, 8)
    for h in range(2):
        cols = slice(h * LANES, (h + 1) * LANES)
        halves = {}
        for p in range(2):
            x2 = [mid[p * 6 + i, rows, cols] for i in range(6)]
            for v in range(3):
                for t in range(2):
                    halves[v, t, p] = sum(w[v, t, q, r] * x2[q * 3 + r] for q in range(2) for r in range(3))
        for t in range(2):
            for u in range(3):
                for s in range(2):
                    out[u, s * 2 + t, rows, cols] = sum(w[u, s, p, v] * halves[v, t, p] for p in range(2) for v in range(3))


def site_tensor(w_ref):
    return {(u, s, p, v): w_ref[((u * 2 + s) * 2 + p) * 3 + v]
            for u in range(3) for s in range(2) for p in range(2) for v in range(3)}


def remote_kernel(own_ref, w_ref, wave, right, part, out, wave_buf, mid):
    own = own_ref[0]
    w = site_tensor(w_ref)

    def run(*refs):
        accs = (refs[:3], refs[3:])

        @pl.when(pl.program_id(0) % 3 == 0)
        def _():
            def split(m, carry):
                for k in range(3):
                    wave_limbs(wave.at[lax.rem(own + 1 + m, 4)], k, wave_buf.at[3 * m + k], CT)
                return carry

            lax.fori_loop(0, 3, split, 0)

        def shard_step(m, carry):
            shard = lax.rem(own + 1 + m, 4)
            reg = 0
            for k in range(3):
                first = pl.multiple_of(shard * 768 + k * BLK, BLK)
                buf = wave_buf.at[3 * m + k]
                reg = first_products(lambda r: right[r, :, pl.ds(first, BLK)], buf, accs, reg)
            return carry

        lax.fori_loop(0, 3, shard_step, 0)
        for r in range(3):
            for p in range(2):
                got = pltpu.matmul_pop(accs[p][r])
                for q in range(2):
                    i = (p * 2 + q) * 3 + r
                    mid[i] = got[q * CT:(q + 1) * CT] + part[i]

        def mix_step(g, carry):
            mix_rows(w, mid, out, pl.multiple_of(g * 8, 8))
            return carry

        lax.fori_loop(0, CT // 8, mix_step, 0)

    pl.run_scoped(run, *acc_refs(2 * CT, 3))


AT = 768


def second_kernel(n_src, width, has_prev, final, *refs):
    lefts, zs, refs = refs[:n_src], refs[n_src:2 * n_src], refs[2 * n_src:]
    prev, refs = (refs[0], refs[1:]) if has_prev else (None, refs)
    out, buf_a, buf_b, zbuf_a, zbuf_b = refs[:5]
    bufs, zbufs = (buf_a, buf_b), (zbuf_a, zbuf_b)
    row, col = pl.program_id(0), pl.program_id(1)
    steps = [(m, u, j * BLK) for m in range(n_src) for u in range(3) for j in range(width // BLK)]

    if final:
        lines, sems = refs[5:]
        turn = row * 3 + col // 2
        slot = lax.rem(turn, 2)

        def copies(turn_of, at):
            first, cols = (turn_of // 3) * AT, lax.rem(turn_of, 3) * 2
            return [
                pltpu.make_async_copy(
                    lines.at[at, half].reshape(AT, 2, 2, LANES),
                    out.at[pl.ds(first, AT), :, :, pl.ds(pl.multiple_of((cols + half) * LANES, LANES), LANES)],
                    sems.at[at, half])
                for half in range(2)
            ]

    def run(acc0, acc1):
        def left_limbs(n):
            m, u, j = steps[n]
            for top in range(0, AT, PIECE):
                for i, limb in enumerate(limbs(lefts[m][u, top:top + PIECE, j:j + BLK])):
                    bufs[n % 2][i, top:top + PIECE] = limb

        def z_limbs(n):
            m, u, j = steps[n]
            for t in range(2):
                for top in range(0, BLK, PIECE):
                    for i, limb in enumerate(limbs(zs[m][u, t, j + top:j + top + PIECE])):
                        zbufs[n % 2][i, t, top:top + PIECE] = limb

        z_limbs(0)
        left_limbs(0)
        reg = 0
        for n in range(len(steps)):
            start = reg
            for t, acc in enumerate((acc0, acc1)):
                reg = full_product(acc, t, [bufs[n % 2][i] for i in range(3)], [zbufs[n % 2][i, t] for i in range(3)], False, start)
            if n + 1 < len(steps):
                z_limbs(n + 1)
                left_limbs(n + 1)
        if final:
            @pl.when((lax.rem(col, 2) == 0) & (turn >= 2))
            def _():
                for copy in copies(turn - 2, slot):
                    copy.wait()

        for t, acc in enumerate((acc0, acc1)):
            got = pltpu.matmul_pop(acc)
            if has_prev:
                got = got + prev[:, t * BLK:(t + 1) * BLK]
            if final:
                for half in range(2):
                    lines[slot, half, pl.ds(2 * lax.rem(col, 2) + t, AT, stride=4), :] = got[:, half * LANES:(half + 1) * LANES]
            else:
                out[:, t * BLK:(t + 1) * BLK] = got

    pl.run_scoped(run, pltpu.ACC(0)((AT, BLK), F32), pltpu.ACC(1)((AT, BLK), F32))

    if final:
        turns = pl.num_programs(0) * 3

        @pl.when(lax.rem(col, 2) == 1)
        def _():
            for copy in copies(turn, slot):
                copy.start()

        @pl.when((lax.rem(col, 2) == 1) & (turn == turns - 1))
        def _():
            for copy in copies(turn - 1, 1 - slot) + copies(turn, slot):
                copy.wait()


def params():
    return pltpu.CompilerParams(vmem_limit_bytes=VMEM_LIMIT)


def cost(flops, nbytes):
    return pl.CostEstimate(flops=flops, bytes_accessed=nbytes, transcendentals=0)


CHUNKS = ((0, 256), (256, 256), (512, 256), (768, 256), (1024, 512))


def solution(mesh):
    def local_apply(wave_blk, left_rows, mpo_ten, right_rows):
        rows_c, cols_f = wave_blk.shape[0], wave_blk.shape[3]
        by, bx = lax.axis_index('by'), lax.axis_index('bx')
        left = left_rows.transpose(1, 0, 2)
        right = right_rows.transpose(1, 0, 2)
        mpo_flat = mpo_ten.reshape(-1)
        own = by.astype(jnp.int32)[None]

        def to_lines(chunks):
            base = chunks[0][0]
            bounds = [((lo - base) // LINE_CT, (lo + n - base) // LINE_CT) for lo, n in chunks]
            return pl.pallas_call(
                lambda *refs: to_lines_kernel(base, bounds, *refs),
                grid=(bounds[-1][1],),
                in_specs=[pl.BlockSpec(memory_space=pl.ANY)],
                out_specs=[pl.BlockSpec((6, LINE_CT * 4, LANES), lambda i, lo=lo, hi=hi: (0, jnp.clip(i - lo, 0, hi - lo - 1), 0)) for lo, hi in bounds],
                out_shape=[jax.ShapeDtypeStruct((6, n * 4, LANES), F32) for _, n in chunks],
                scratch_shapes=[pltpu.SemaphoreType.DMA((6,))],
                compiler_params=params(),
                cost_estimate=cost(10**9 * bounds[-1][1], bounds[-1][1] * 4 * 2**20),
                name='to_lines',
            )(wave_blk)

        lines = to_lines(CHUNKS[:1]) + to_lines(CHUNKS[1:])
        gathered = [lax.all_gather(line, 'by', axis=0, tiled=False) for line in lines]

        part = pl.pallas_call(
            lambda idx, *refs: local_kernel(rows_c // CT, *refs),
            grid_spec=pltpu.PrefetchScalarGridSpec(
                num_scalar_prefetch=1,
                grid=(rows_c // CT,),
                in_specs=[
                    pl.BlockSpec(memory_space=pl.ANY),
                    pl.BlockSpec((3, 768, 768), lambda i, idx: (0, 0, idx[0]), pipeline_mode=pl.Buffered(1)),
                ],
                out_specs=pl.BlockSpec((12, CT, 768), lambda i, idx: (0, i, 0)),
                scratch_shapes=[pltpu.VMEM((2, 6, CT * 4, LANES), F32), pltpu.SemaphoreType.DMA((2, 6))]
                + [pltpu.VMEM((3, 2, 2 * CT, BLK), BF16)] * 3,
            ),
            out_shape=jax.ShapeDtypeStruct((12, rows_c, 768), F32),
            compiler_params=params(),
            cost_estimate=cost(2 * rows_c * 4 * 768 * 2304 * 6, 120 * 2**20),
            name='local_part',
        )(own, wave_blk, right)

        def first(k, got):
            lo, n = CHUNKS[k]
            tiles = n // CT
            return pl.pallas_call(
                remote_kernel,
                grid_spec=pltpu.PrefetchScalarGridSpec(
                    num_scalar_prefetch=1,
                    grid=(tiles * 3,),
                    in_specs=[
                        pl.BlockSpec(memory_space=pltpu.SMEM),
                        pl.BlockSpec((4, 6, CT * 4, LANES), lambda i, idx: (0, 0, i // 3, 0)),
                        pl.BlockSpec((3, BLK, 3072), lambda i, idx: (0, i % 3, 0)),
                        pl.BlockSpec((12, CT, BLK), lambda i, idx: (0, lo // CT + i // 3, i % 3)),
                    ],
                    out_specs=pl.BlockSpec((3, 4, CT, BLK), lambda i, idx: (0, 0, i // 3, i % 3)),
                    scratch_shapes=[pltpu.VMEM((9, 3, 2, 2 * CT, BLK), BF16), pltpu.VMEM((12, CT, BLK), F32)],
                ),
                out_shape=jax.ShapeDtypeStruct((3, 4, n, 768), F32),
                compiler_params=params(),
                cost_estimate=cost(2 * n * 4 * 2304 * 2304 * 6, 60 * 2**20),
                name='remote_part',
            )(own, mpo_flat, got, right, part)

        def second(group, mine, theirs, prev, final):
            width = CHUNKS[group[0]][1]
            srcs = [(bx, k) for k in group] + [(1 - bx, k) for k in group]
            where = jnp.stack([(b * rows_c + CHUNKS[k][0]) // width for b, k in srcs]).astype(jnp.int32)
            n_src = len(srcs)
            in_specs = [pl.BlockSpec((3, AT, width), lambda a, n, idx, m=m: (0, a, idx[m])) for m in range(n_src)]
            in_specs += [pl.BlockSpec((3, 2, width, BLK), lambda a, n, idx: (0, n % 2, 0, n // 2))] * n_src
            operands = [left] * n_src + mine + theirs
            if prev is not None:
                in_specs.append(pl.BlockSpec((AT, 2 * BLK), lambda a, n, idx: (a, n)))
                operands.append(prev)
            scratch = [pltpu.VMEM((3, AT, BLK), BF16)] * 2 + [pltpu.VMEM((3, 2, BLK, BLK), BF16)] * 2
            if final:
                out_spec = pl.BlockSpec(memory_space=pl.ANY)
                out_shape = jax.ShapeDtypeStruct((rows_c, 2, 2, cols_f), F32)
                scratch += [pltpu.VMEM((2, 2, AT * 4, LANES), F32), pltpu.SemaphoreType.DMA((2, 2))]
            else:
                out_spec = pl.BlockSpec((AT, 2 * BLK), lambda a, n, idx: (a, n))
                out_shape = jax.ShapeDtypeStruct((rows_c, 3072), F32)
            return pl.pallas_call(
                lambda idx, *refs: second_kernel(n_src, width, prev is not None, final, *refs),
                grid_spec=pltpu.PrefetchScalarGridSpec(
                    num_scalar_prefetch=1,
                    grid=(rows_c // AT, 6),
                    in_specs=in_specs,
                    out_specs=out_spec,
                    scratch_shapes=scratch,
                ),
                out_shape=out_shape,
                compiler_params=params(),
                cost_estimate=cost(2 * rows_c * 3072 * 3 * width * n_src * 6, 100 * 2**20),
                name='second_part',
            )(where, *operands)

        mine, theirs = [], []

        def stage(k):
            z = first(k, gathered[k])
            mine.append(z)
            theirs.append(lax.ppermute(z, 'bx', [(0, 1), (1, 0)]))

        def apply(group, prev, final):
            return second(group, [mine[k] for k in group], [theirs[k] for k in group], prev, final)

        def after(k, val):
            gathered[k], val = lax.optimization_barrier((gathered[k], val))
            return val

        stage(0)
        stage(1)
        acc = apply([0], None, False)
        acc = after(2, acc)
        stage(2)
        stage(3)
        acc = apply([1, 2], acc, False)
        acc = after(4, acc)
        stage(4)
        acc, mine[4] = lax.optimization_barrier((acc, mine[4]))
        acc = apply([3], acc, False)
        return apply([4], acc, True)

    return jax.shard_map(local_apply, mesh=mesh, in_specs=(P('bx', None, None, 'by'), P('bx', None, None), P(), P('by', None, None)), out_specs=P('bx', None, None, 'by'), check_vma=False)
```

```python
import jax
import jax.numpy as jnp
from jax import lax
from jax.experimental import pallas as pl
from jax.experimental.pallas import tpu as pltpu
from jax.sharding import PartitionSpec as P

F32 = jnp.float32
BF16 = jnp.bfloat16
LANES = 128
BLK = 256
VMEM_LIMIT = 62 * 2**20


def limbs(val):
    hi = val.astype(BF16)
    rest = val - hi.astype(F32)
    mid = rest.astype(BF16)
    return hi, mid, (rest - mid.astype(F32)).astype(BF16)


def full_product(acc, unit, lhs_limbs, rhs_limbs, transpose, reg):
    for depth, rhs in enumerate(rhs_limbs):
        pltpu.matmul_push_rhs(rhs, staging_register=reg, mxu_index=unit, transpose=transpose)
        for i in range(3 - depth):
            pltpu.matmul_acc_lhs(acc, lhs_limbs[i], load_staged_rhs=reg if i == 0 else None)
        reg = 1 - reg
    return reg


PIECE = 64


def wave_limbs(lines, k, buf, rows):
    for p in range(2):
        for q in range(2):
            for top in range(0, rows, PIECE):
                for half in range(2):
                    part = lines[2 * k + half, pl.ds(4 * top + 2 * p + q, PIECE, stride=4), :]
                    for i, limb in enumerate(limbs(part)):
                        buf[i, p, q * rows + top:q * rows + top + PIECE, half * LANES:(half + 1) * LANES] = limb


def first_products(env_of, buf, accs, reg):
    for r in range(3):
        env = limbs(env_of(r))
        start = reg
        for p in range(2):
            reg = full_product(accs[p][r], p, [buf[i, p] for i in range(3)], env, True, start)
    return reg


def acc_refs(rows, count):
    return tuple(pltpu.ACC(unit)((rows, BLK), F32) for unit in range(2) for _ in range(count))


CT = 128
LINE_CT = 128


def line_copies(wave, first, rows, lines, sems):
    return [
        pltpu.make_async_copy(
            wave.at[pl.ds(first, rows), :, :, pl.ds(f * LANES, LANES)], lines.at[f].reshape(rows, 2, 2, LANES), sems.at[f])
        for f in range(6)
    ]


def to_lines_kernel(base, bounds, wave, *refs):
    outs, sems = refs[:-1], refs[-1]
    step = pl.program_id(0)
    for out, (lo, hi) in zip(outs, bounds):
        @pl.when((step >= lo) & (step < hi))
        def _():
            copies = line_copies(wave, base + step * LINE_CT, LINE_CT, out, sems)
            for copy in copies:
                copy.start()
            for copy in copies:
                copy.wait()


def local_kernel(n_tiles, wave, right, part, lines, sems, buf_a, buf_b, buf_c):
    bufs = (buf_a, buf_b, buf_c)
    step = pl.program_id(0)
    slot = lax.rem(step, 2)

    def copies(tile, at):
        return line_copies(wave, tile * CT, CT, lines.at[at], sems.at[at])

    @pl.when(step == 0)
    def _():
        for copy in copies(0, 0):
            copy.start()

    @pl.when(step + 1 < n_tiles)
    def _():
        for copy in copies(step + 1, 1 - slot):
            copy.start()

    for copy in copies(step, slot):
        copy.wait()
    here = lines.at[slot]

    def run(*refs):
        accs = (refs[:3], refs[3:])
        reg = 0
        wave_limbs(here, 0, bufs[0], CT)
        for b in range(3):
            for k in range(3):
                if b == 0 and k < 2:
                    wave_limbs(here, k + 1, bufs[k + 1], CT)
                reg = first_products(lambda r: right[r, b * BLK:(b + 1) * BLK, k * BLK:(k + 1) * BLK], bufs[k], accs, reg)
            for r in range(3):
                for p in range(2):
                    got = pltpu.matmul_pop(accs[p][r])
                    for q in range(2):
                        part[(p * 2 + q) * 3 + r, :, b * BLK:(b + 1) * BLK] = got[q * CT:(q + 1) * CT]

    pl.run_scoped(run, *acc_refs(2 * CT, 3))


def mix_rows(w, mid, out, row):
    rows = pl.ds(row, 8)
    for h in range(2):
        cols = slice(h * LANES, (h + 1) * LANES)
        halves = {}
        for p in range(2):
            x2 = [mid[p * 6 + i, rows, cols] for i in range(6)]
            for v in range(3):
                for t in range(2):
                    halves[v, t, p] = sum(w[v, t, q, r] * x2[q * 3 + r] for q in range(2) for r in range(3))
        for t in range(2):
            for u in range(3):
                for s in range(2):
                    out[u, s * 2 + t, rows, cols] = sum(w[u, s, p, v] * halves[v, t, p] for p in range(2) for v in range(3))


def site_tensor(w_ref):
    return {(u, s, p, v): w_ref[((u * 2 + s) * 2 + p) * 3 + v]
            for u in range(3) for s in range(2) for p in range(2) for v in range(3)}


def remote_kernel(own_ref, w_ref, wave, right, part, out, wave_buf, mid):
    own = own_ref[0]
    w = site_tensor(w_ref)

    def run(*refs):
        accs = (refs[:3], refs[3:])

        @pl.when(pl.program_id(0) % 3 == 0)
        def _():
            def split(m, carry):
                for k in range(3):
                    wave_limbs(wave.at[lax.rem(own + 1 + m, 4)], k, wave_buf.at[3 * m + k], CT)
                return carry

            lax.fori_loop(0, 3, split, 0)

        def shard_step(m, carry):
            shard = lax.rem(own + 1 + m, 4)
            reg = 0
            for k in range(3):
                first = pl.multiple_of(shard * 768 + k * BLK, BLK)
                buf = wave_buf.at[3 * m + k]
                reg = first_products(lambda r: right[r, :, pl.ds(first, BLK)], buf, accs, reg)
            return carry

        lax.fori_loop(0, 3, shard_step, 0)
        for r in range(3):
            for p in range(2):
                got = pltpu.matmul_pop(accs[p][r])
                for q in range(2):
                    i = (p * 2 + q) * 3 + r
                    mid[i] = got[q * CT:(q + 1) * CT] + part[i]

        def mix_step(g, carry):
            mix_rows(w, mid, out, pl.multiple_of(g * 8, 8))
            return carry

        lax.fori_loop(0, CT // 8, mix_step, 0)

    pl.run_scoped(run, *acc_refs(2 * CT, 3))


AT = 768


def second_kernel(n_src, width, has_prev, final, *refs):
    lefts, zs, refs = refs[:n_src], refs[n_src:2 * n_src], refs[2 * n_src:]
    prev, refs = (refs[0], refs[1:]) if has_prev else (None, refs)
    out, buf_a, buf_b, zbuf_a, zbuf_b = refs[:5]
    bufs, zbufs = (buf_a, buf_b), (zbuf_a, zbuf_b)
    row, col = pl.program_id(0), pl.program_id(1)
    steps = [(m, u, j * BLK) for m in range(n_src) for u in range(3) for j in range(width // BLK)]

    if final:
        lines, sems = refs[5:]
        turn = row * 3 + col // 2
        slot = lax.rem(turn, 2)

        def copies(turn_of, at):
            first, cols = (turn_of // 3) * AT, lax.rem(turn_of, 3) * 2
            return [
                pltpu.make_async_copy(
                    lines.at[at, half].reshape(AT, 2, 2, LANES),
                    out.at[pl.ds(first, AT), :, :, pl.ds(pl.multiple_of((cols + half) * LANES, LANES), LANES)],
                    sems.at[at, half])
                for half in range(2)
            ]

    def run(acc0, acc1):
        def left_limbs(n):
            m, u, j = steps[n]
            for top in range(0, AT, PIECE):
                for i, limb in enumerate(limbs(lefts[m][u, top:top + PIECE, j:j + BLK])):
                    bufs[n % 2][i, top:top + PIECE] = limb

        def z_limbs(n):
            m, u, j = steps[n]
            for t in range(2):
                for top in range(0, BLK, PIECE):
                    for i, limb in enumerate(limbs(zs[m][u, t, j + top:j + top + PIECE])):
                        zbufs[n % 2][i, t, top:top + PIECE] = limb

        z_limbs(0)
        left_limbs(0)
        reg = 0
        for n in range(len(steps)):
            start = reg
            for t, acc in enumerate((acc0, acc1)):
                reg = full_product(acc, t, [bufs[n % 2][i] for i in range(3)], [zbufs[n % 2][i, t] for i in range(3)], False, start)
            if n + 1 < len(steps):
                z_limbs(n + 1)
                left_limbs(n + 1)
        if final:
            @pl.when((lax.rem(col, 2) == 0) & (turn >= 2))
            def _():
                for copy in copies(turn - 2, slot):
                    copy.wait()

        for t, acc in enumerate((acc0, acc1)):
            got = pltpu.matmul_pop(acc)
            if has_prev:
                got = got + prev[:, t * BLK:(t + 1) * BLK]
            if final:
                for half in range(2):
                    lines[slot, half, pl.ds(2 * lax.rem(col, 2) + t, AT, stride=4), :] = got[:, half * LANES:(half + 1) * LANES]
            else:
                out[:, t * BLK:(t + 1) * BLK] = got

    pl.run_scoped(run, pltpu.ACC(0)((AT, BLK), F32), pltpu.ACC(1)((AT, BLK), F32))

    if final:
        turns = pl.num_programs(0) * 3

        @pl.when(lax.rem(col, 2) == 1)
        def _():
            for copy in copies(turn, slot):
                copy.start()

        @pl.when((lax.rem(col, 2) == 1) & (turn == turns - 1))
        def _():
            for copy in copies(turn - 1, 1 - slot) + copies(turn, slot):
                copy.wait()


def params():
    return pltpu.CompilerParams(vmem_limit_bytes=VMEM_LIMIT)


def cost(flops, nbytes):
    return pl.CostEstimate(flops=flops, bytes_accessed=nbytes, transcendentals=0)


CHUNKS = ((0, 256), (256, 256), (512, 256), (768, 256), (1024, 512))


def solution(mesh):
    def local_apply(wave_blk, left_rows, mpo_ten, right_rows):
        rows_c, cols_f = wave_blk.shape[0], wave_blk.shape[3]
        by, bx = lax.axis_index('by'), lax.axis_index('bx')
        left = left_rows.transpose(1, 0, 2)
        right = right_rows.transpose(1, 0, 2)
        mpo_flat = mpo_ten.reshape(-1)
        own = by.astype(jnp.int32)[None]

        def to_lines(chunks):
            base = chunks[0][0]
            bounds = [((lo - base) // LINE_CT, (lo + n - base) // LINE_CT) for lo, n in chunks]
            return pl.pallas_call(
                lambda *refs: to_lines_kernel(base, bounds, *refs),
                grid=(bounds[-1][1],),
                in_specs=[pl.BlockSpec(memory_space=pl.ANY)],
                out_specs=[pl.BlockSpec((6, LINE_CT * 4, LANES), lambda i, lo=lo, hi=hi: (0, jnp.clip(i - lo, 0, hi - lo - 1), 0)) for lo, hi in bounds],
                out_shape=[jax.ShapeDtypeStruct((6, n * 4, LANES), F32) for _, n in chunks],
                scratch_shapes=[pltpu.SemaphoreType.DMA((6,))],
                compiler_params=params(),
                cost_estimate=cost(10**9 * bounds[-1][1], bounds[-1][1] * 4 * 2**20),
                name='to_lines',
            )(wave_blk)

        lines = to_lines(CHUNKS[:1]) + to_lines(CHUNKS[1:])
        gathered = [lax.all_gather(line, 'by', axis=0, tiled=False) for line in lines]

        part = pl.pallas_call(
            lambda idx, *refs: local_kernel(rows_c // CT, *refs),
            grid_spec=pltpu.PrefetchScalarGridSpec(
                num_scalar_prefetch=1,
                grid=(rows_c // CT,),
                in_specs=[
                    pl.BlockSpec(memory_space=pl.ANY),
                    pl.BlockSpec((3, 768, 768), lambda i, idx: (0, 0, idx[0]), pipeline_mode=pl.Buffered(1)),
                ],
                out_specs=pl.BlockSpec((12, CT, 768), lambda i, idx: (0, i, 0)),
                scratch_shapes=[pltpu.VMEM((2, 6, CT * 4, LANES), F32), pltpu.SemaphoreType.DMA((2, 6))]
                + [pltpu.VMEM((3, 2, 2 * CT, BLK), BF16)] * 3,
            ),
            out_shape=jax.ShapeDtypeStruct((12, rows_c, 768), F32),
            compiler_params=params(),
            cost_estimate=cost(2 * rows_c * 4 * 768 * 2304 * 6, 120 * 2**20),
            name='local_part',
        )(own, wave_blk, right)

        def first(k, got):
            lo, n = CHUNKS[k]
            tiles = n // CT
            return pl.pallas_call(
                remote_kernel,
                grid_spec=pltpu.PrefetchScalarGridSpec(
                    num_scalar_prefetch=1,
                    grid=(tiles * 3,),
                    in_specs=[
                        pl.BlockSpec(memory_space=pltpu.SMEM),
                        pl.BlockSpec((4, 6, CT * 4, LANES), lambda i, idx: (0, 0, i // 3, 0)),
                        pl.BlockSpec((3, BLK, 3072), lambda i, idx: (0, i % 3, 0)),
                        pl.BlockSpec((12, CT, BLK), lambda i, idx: (0, lo // CT + i // 3, i % 3)),
                    ],
                    out_specs=pl.BlockSpec((3, 4, CT, BLK), lambda i, idx: (0, 0, i // 3, i % 3)),
                    scratch_shapes=[pltpu.VMEM((9, 3, 2, 2 * CT, BLK), BF16), pltpu.VMEM((12, CT, BLK), F32)],
                ),
                out_shape=jax.ShapeDtypeStruct((3, 4, n, 768), F32),
                compiler_params=params(),
                cost_estimate=cost(2 * n * 4 * 2304 * 2304 * 6, 60 * 2**20),
                name='remote_part',
            )(own, mpo_flat, got, right, part)

        def second(group, mine, theirs, prev, final):
            width = CHUNKS[group[0]][1]
            srcs = [(bx, k) for k in group] + [(1 - bx, k) for k in group]
            where = jnp.stack([(b * rows_c + CHUNKS[k][0]) // width for b, k in srcs]).astype(jnp.int32)
            n_src = len(srcs)
            in_specs = [pl.BlockSpec((3, AT, width), lambda a, n, idx, m=m: (0, a, idx[m])) for m in range(n_src)]
            in_specs += [pl.BlockSpec((3, 2, width, BLK), lambda a, n, idx: (0, n % 2, 0, n // 2))] * n_src
            operands = [left] * n_src + mine + theirs
            if prev is not None:
                in_specs.append(pl.BlockSpec((AT, 2 * BLK), lambda a, n, idx: (a, n)))
                operands.append(prev)
            scratch = [pltpu.VMEM((3, AT, BLK), BF16)] * 2 + [pltpu.VMEM((3, 2, BLK, BLK), BF16)] * 2
            if final:
                out_spec = pl.BlockSpec(memory_space=pl.ANY)
                out_shape = jax.ShapeDtypeStruct((rows_c, 2, 2, cols_f), F32)
                scratch += [pltpu.VMEM((2, 2, AT * 4, LANES), F32), pltpu.SemaphoreType.DMA((2, 2))]
            else:
                out_spec = pl.BlockSpec((AT, 2 * BLK), lambda a, n, idx: (a, n))
                out_shape = jax.ShapeDtypeStruct((rows_c, 3072), F32)
            return pl.pallas_call(
                lambda idx, *refs: second_kernel(n_src, width, prev is not None, final, *refs),
                grid_spec=pltpu.PrefetchScalarGridSpec(
                    num_scalar_prefetch=1,
                    grid=(rows_c // AT, 6),
                    in_specs=in_specs,
                    out_specs=out_spec,
                    scratch_shapes=scratch,
                ),
                out_shape=out_shape,
                compiler_params=params(),
                cost_estimate=cost(2 * rows_c * 3072 * 3 * width * n_src * 6, 100 * 2**20),
                name='second_part',
            )(where, *operands)

        mine, theirs = [], []

        def stage(k):
            z = first(k, gathered[k])
            mine.append(z)
            theirs.append(lax.ppermute(z, 'bx', [(0, 1), (1, 0)]))

        def apply(group, prev, final):
            return second(group, [mine[k] for k in group], [theirs[k] for k in group], prev, final)

        def before(k, val):
            gathered[k], val = lax.optimization_barrier((gathered[k], val))
            return val

        def behind(k, val):
            val, mine[k] = lax.optimization_barrier((val, mine[k]))
            return val

        stage(0)
        stage(1)
        mine[0] = behind(1, mine[0])
        acc = apply([0], None, False)
        acc = before(2, acc)
        stage(2)
        mine[2] = before(3, mine[2])
        stage(3)
        acc = behind(3, acc)
        acc = apply([1, 2], acc, False)
        acc = before(4, acc)
        gathered[4], theirs[3] = lax.optimization_barrier((gathered[4], theirs[3]))
        stage(4)
        acc = behind(4, acc)
        acc = apply([3], acc, False)
        return apply([4], acc, True)

    return jax.shard_map(local_apply, mesh=mesh, in_specs=(P('bx', None, None, 'by'), P('bx', None, None), P(), P('by', None, None)), out_specs=P('bx', None, None, 'by'), check_vma=False)
```
